32 devices in a mesh: dp: 1, sp: 32 (over x, y, z, core).
Axes of the slice: x: 2, y: 2, z: 4, core: 2. Of those that a mesh axis runs over, the one named last changes fastest.
Arguments:
- q: bfloat16 [32, 8, 256], P('dp')
- k: bfloat16 [32, 8192, 8, 256], P('dp', 'sp')
- v: bfloat16 [32, 8192, 8, 256], P('dp', 'sp')
Outputs:
- q: bfloat16 [32, 8, 256], P('dp')
All inputs are finite; a program needn't handle non-finite values.
Results may differ from the reference program's by a relative error of at most 0.012.
Values are sent between devices in bfloat16 or wider.
A program may use at most 2 GiB of HBM per device.

```python
import jax
import jax.numpy as jnp

BATCH = 32
CACHE = 8192
HEADS = 8
KV_HEADS = 8
HEAD = 256


def setup_inputs(seed: int = 0, part: int = 0) -> dict:
    kq, kk, kv = (jax.random.fold_in(k, part) for k in jax.random.split(jax.random.key(seed), 3))
    return {
        "q": (3 * jax.random.normal(kq, (BATCH, HEADS, HEAD), jnp.float32)).astype(jnp.bfloat16),
        "k": jax.random.normal(kk, (BATCH, CACHE, KV_HEADS, HEAD), jnp.float32).astype(jnp.bfloat16),
        "v": jax.random.normal(kv, (BATCH, CACHE, KV_HEADS, HEAD), jnp.float32).astype(jnp.bfloat16),
    }


def einsum(form, a, b):
    return jnp.einsum(form, a.astype(jnp.float32), b.astype(jnp.float32))


def reference(q, k, v):
    grouped = q.reshape(BATCH, KV_HEADS, -1, HEAD)
    scores = einsum("bgsd,bugd->bgsu", grouped, k) * HEAD**-0.5
    weights = jax.nn.softmax(scores, -1).astype(jnp.bfloat16)
    return einsum("bgsu,bugd->bgsd", weights, v).astype(jnp.bfloat16).reshape(BATCH, HEADS, HEAD)
```

```python
import functools

import jax
import jax.numpy as jnp
from jax import lax
from jax.experimental import pallas as pl
from jax.experimental.pallas import tpu as pltpu
from jax.sharding import PartitionSpec as P

SLOTS = 8
LAG = 6


def flip(index, mask, bits):
    out = 0
    for bit in range(bits):
        a, b = index // 2**bit % 2, mask // 2**bit % 2
        out = out + 2**bit * (a + b - 2 * a * b)
    return out


def kernel(n, bits, q_hbm, k_hbm, v_hbm, out, q, k, v, seen, stats, seen_in, stats_in, q_sem, k_sem, v_sem, send_sem, recv_sem, out_send, out_recv):
    me = lax.axis_index("sp")
    seqs = q.shape[0]

    def owner(step):
        return flip(me, n - 1 - step, bits)

    def load(hbm, buf, sem, step):
        slot = lax.rem(step, SLOTS)
        return pltpu.make_async_copy(hbm.at[owner(step)], buf.at[slot], sem.at[slot])

    q_copy = pltpu.make_async_copy(q_hbm, q, q_sem)
    q_copy.start()

    @pl.loop(0, SLOTS)
    def _(step):
        load(k_hbm, k, k_sem, step).start()
        load(v_hbm, v, v_sem, step).start()

    barrier = pltpu.get_barrier_semaphore()

    @pl.loop(1, n)
    def _(hop):
        pl.semaphore_signal(barrier, inc=1, device_id={"sp": lax.rem(me + hop, n)}, device_id_type=pl.DeviceIdType.MESH)

    q_copy.wait()

    heads, head = q.shape[1:]
    lane = lax.broadcasted_iota(jnp.int32, (heads, k.shape[1] * heads), 1)
    own = lane % heads == lax.broadcasted_iota(jnp.int32, lane.shape, 0)

    def scores(step):
        load(k_hbm, k, k_sem, step).wait()
        keys = k[lax.rem(step, SLOTS)].reshape(-1, head)
        s = lax.dot_general(q[owner(step)], keys, (((1,), (1,)), ((), ())), preferred_element_type=jnp.float32) * head**-0.5
        s = jnp.where(own, s, -jnp.inf)
        high = jnp.max(s, -1, keepdims=True)
        w = jnp.exp(s - high)
        return w.astype(jnp.bfloat16), high, jnp.sum(w, -1, keepdims=True)

    def values(step, w):
        load(v_hbm, v, v_sem, step).wait()
        vals = v[lax.rem(step, SLOTS)].reshape(-1, head)
        return lax.dot_general(w, vals, (((1,), (0,)), ((), ())), preferred_element_type=jnp.float32)

    def keep(step, o, high, total):
        seen[step] = o.astype(jnp.bfloat16)
        stats[step] = jnp.concatenate([jnp.broadcast_to(high, (heads, 128)), jnp.broadcast_to(total, (heads, 128))], -1)

    def send(step):
        to = owner(step)
        args = dict(device_id={"sp": to}, device_id_type=pl.DeviceIdType.MESH)
        return (
            pltpu.make_async_remote_copy(seen.at[step], seen_in.at[step], send_sem.at[0], recv_sem.at[0], **args),
            pltpu.make_async_remote_copy(stats.at[step], stats_in.at[step], send_sem.at[1], recv_sem.at[1], **args),
        )

    def body(step, carry):
        w, high, total = carry
        new = scores(step)
        o = values(step - 1, w)
        keep(step - 1, o, high, total)

        @pl.when(step + SLOTS < n)
        def _():
            load(k_hbm, k, k_sem, step + SLOTS).start()

        @pl.when(step - 1 + SLOTS < n)
        def _():
            load(v_hbm, v, v_sem, step - 1 + SLOTS).start()

        @pl.when(step == LAG)
        def _():
            pl.semaphore_wait(barrier, n - 1)

            @pl.loop(0, LAG - 1)
            def _(earlier):
                for copy in send(earlier):
                    copy.start()

        @pl.when(step >= LAG)
        def _():
            for copy in send(step - 1):
                copy.start()

        return new

    first = scores(0)

    @pl.when(SLOTS < n)
    def _():
        load(k_hbm, k, k_sem, SLOTS).start()

    w, high, total = lax.fori_loop(1, n, body, first)
    o = values(n - 1, w)

    pltpu.make_async_copy(seen_in.at[pl.ds(0, n - 1)], seen_in.at[pl.ds(0, n - 1)], recv_sem.at[0]).wait()
    pltpu.make_async_copy(stats_in.at[pl.ds(0, n - 1)], stats_in.at[pl.ds(0, n - 1)], recv_sem.at[1]).wait()
    highs = [stats_in[i, :, :128] for i in range(n - 1)] + [jnp.broadcast_to(high, (heads, 128))]
    totals = [stats_in[i, :, 128:] for i in range(n - 1)] + [jnp.broadcast_to(total, (heads, 128))]
    parts = [seen_in[i] for i in range(n - 1)] + [o]
    top = functools.reduce(jnp.maximum, highs)
    scale = [jnp.exp(x - top) for x in highs]
    bottom = functools.reduce(jnp.add, [x * y for x, y in zip(scale, totals)])
    wide = lambda x: jnp.concatenate([x] * (head // 128), -1)
    upper = functools.reduce(jnp.add, [wide(x) * y.astype(jnp.float32) for x, y in zip(scale, parts)])
    out[me] = (upper / wide(bottom)).astype(jnp.bfloat16)

    def result(hop):
        return pltpu.make_async_remote_copy(out.at[me], out.at[me], out_send, out_recv, device_id={"sp": flip(me, hop, bits)}, device_id_type=pl.DeviceIdType.MESH)

    @pl.loop(0, n - 1)
    def _(hop):
        result(n - 1 - hop).start()

    pltpu.make_async_copy(seen.at[pl.ds(0, n - 1)], seen.at[pl.ds(0, n - 1)], send_sem.at[0]).wait()
    pltpu.make_async_copy(stats.at[pl.ds(0, n - 1)], stats.at[pl.ds(0, n - 1)], send_sem.at[1]).wait()
    pltpu.make_async_copy(out.at[pl.ds(0, n - 1)], out.at[pl.ds(0, n - 1)], out_send).wait()
    pltpu.make_async_copy(out.at[pl.ds(0, n - 1)], out.at[pl.ds(0, n - 1)], out_recv).wait()


def solution(mesh):
    n = mesh.shape["sp"]

    def step(q, k, v):
        seqs, tokens, heads, head = k.shape
        return pl.pallas_call(
            functools.partial(kernel, n, (n - 1).bit_length()),
            out_shape=jax.ShapeDtypeStruct(q.shape, q.dtype),
            in_specs=[pl.BlockSpec(memory_space=pl.ANY)] * 3,
            out_specs=pl.BlockSpec(memory_space=pltpu.VMEM),
            scratch_shapes=[
                pltpu.VMEM(q.shape, q.dtype),
                pltpu.VMEM((SLOTS, tokens, heads, head), k.dtype),
                pltpu.VMEM((SLOTS, tokens, heads, head), v.dtype),
                pltpu.VMEM((n, heads, head), jnp.bfloat16),
                pltpu.VMEM((n, heads, 256), jnp.float32),
                pltpu.VMEM((n, heads, head), jnp.bfloat16),
                pltpu.VMEM((n, heads, 256), jnp.float32),
                pltpu.SemaphoreType.DMA,
                pltpu.SemaphoreType.DMA((SLOTS,)),
                pltpu.SemaphoreType.DMA((SLOTS,)),
                pltpu.SemaphoreType.DMA((2,)),
                pltpu.SemaphoreType.DMA((2,)),
                pltpu.SemaphoreType.DMA,
                pltpu.SemaphoreType.DMA,
            ],
            compiler_params=pltpu.CompilerParams(collective_id=0, has_side_effects=True, vmem_limit_bytes=60 * 2**20),
        )(q, k, v)

    return jax.shard_map(
        step,
        mesh=mesh,
        in_specs=(P("dp", None, None), P("dp", "sp", None, None), P("dp", "sp", None, None)),
        out_specs=P("dp", None, None),
        check_vma=False,
    )
```

```python
import functools

import jax
import jax.numpy as jnp
from jax import lax
from jax.experimental import pallas as pl
from jax.experimental.pallas import tpu as pltpu
from jax.sharding import PartitionSpec as P

SLOTS = 8
LAG = 6


def kernel(n, q_hbm, k_hbm, v_hbm, out, q, k, v, raw, weights, seen, stats, seen_in, stats_in, q_sem, k_sem, v_sem, send_sem, recv_sem, out_send, out_recv):
    me = lax.axis_index("sp")
    seqs = q.shape[0]

    def owner(step):
        return lax.bitwise_xor(me, n - 1 - step)

    def load(hbm, buf, sem, step):
        slot = lax.rem(step, SLOTS)
        return pltpu.make_async_copy(hbm.at[owner(step)], buf.at[slot], sem.at[slot])

    q_copy = pltpu.make_async_copy(q_hbm, q, q_sem)
    q_copy.start()

    @pl.loop(0, SLOTS)
    def _(step):
        load(k_hbm, k, k_sem, step).start()
        load(v_hbm, v, v_sem, step).start()

    barrier = pltpu.get_barrier_semaphore()

    @pl.loop(1, n)
    def _(hop):
        pl.semaphore_signal(barrier, inc=1, device_id={"sp": lax.rem(me + hop, n)}, device_id_type=pl.DeviceIdType.MESH)

    q_copy.wait()

    heads, head = q.shape[1:]
    lane = lax.broadcasted_iota(jnp.int32, (heads, k.shape[1] * heads), 1)
    own = lane % heads == lax.broadcasted_iota(jnp.int32, lane.shape, 0)

    def scores(step):
        keys = k[lax.rem(step, SLOTS)].reshape(-1, head)
        return lax.dot_general(q[owner(step)], keys, (((1,), (1,)), ((), ())), preferred_element_type=jnp.float32)

    def soften(step, s):
        s = jnp.where(own, s * head**-0.5, -jnp.inf)
        high = jnp.max(s, -1, keepdims=True)
        w = jnp.exp(s - high)
        total = jnp.sum(w, -1, keepdims=True)
        stats[step] = jnp.concatenate([jnp.broadcast_to(high, (heads, 128)), jnp.broadcast_to(total, (heads, 128))], -1)
        return w.astype(jnp.bfloat16)

    def values(step, w):
        vals = v[lax.rem(step, SLOTS)].reshape(-1, head)
        half = vals.shape[0] // 2
        dot = lambda a, b: lax.dot_general(a, b, (((1,), (0,)), ((), ())), preferred_element_type=jnp.float32)
        return dot(w[:, :half], vals[:half]) + dot(w[:, half:], vals[half:])

    def send(step):
        to = owner(step)
        args = dict(device_id={"sp": to}, device_id_type=pl.DeviceIdType.MESH)
        return (
            pltpu.make_async_remote_copy(seen.at[step], seen_in.at[step], send_sem.at[0], recv_sem.at[0], **args),
            pltpu.make_async_remote_copy(stats.at[step], stats_in.at[step], send_sem.at[1], recv_sem.at[1], **args),
        )

    def wait(hbm, buf, sem, step):
        load(hbm, buf, sem, step).wait()

    def refill(hbm, buf, sem, step):
        @pl.when(step + SLOTS < n)
        def _():
            load(hbm, buf, sem, step + SLOTS).start()

    wait(k_hbm, k, k_sem, 0)
    raw[...] = scores(0)
    refill(k_hbm, k, k_sem, 0)
    wait(k_hbm, k, k_sem, 1)
    old = raw[...]
    raw[...] = scores(1)
    weights[...] = soften(0, old)
    refill(k_hbm, k, k_sem, 1)

    @pl.loop(2, n)
    def _(step):
        wait(v_hbm, v, v_sem, step - 2)
        wait(k_hbm, k, k_sem, step)
        old, w = raw[...], weights[...]
        new = scores(step)
        o = values(step - 2, w)
        weights[...] = soften(step - 1, old)
        raw[...] = new
        seen[step - 2] = o.astype(jnp.bfloat16)
        refill(v_hbm, v, v_sem, step - 2)
        refill(k_hbm, k, k_sem, step)

        @pl.when(step == LAG)
        def _():
            pl.semaphore_wait(barrier, n - 1)

            @pl.loop(0, LAG - 2)
            def _(earlier):
                for copy in send(earlier):
                    copy.start()

        @pl.when(step >= LAG)
        def _():
            for copy in send(step - 2):
                copy.start()

    w = weights[...]
    weights[...] = soften(n - 1, raw[...])
    wait(v_hbm, v, v_sem, n - 2)
    seen[n - 2] = values(n - 2, w).astype(jnp.bfloat16)
    for copy in send(n - 2):
        copy.start()
    wait(v_hbm, v, v_sem, n - 1)
    o = values(n - 1, weights[...])
    high, total = stats[n - 1, :, :128], stats[n - 1, :, 128:]

    pltpu.make_async_copy(seen_in.at[pl.ds(0, n - 1)], seen_in.at[pl.ds(0, n - 1)], recv_sem.at[0]).wait()
    pltpu.make_async_copy(stats_in.at[pl.ds(0, n - 1)], stats_in.at[pl.ds(0, n - 1)], recv_sem.at[1]).wait()
    highs = [stats_in[i, :, :128] for i in range(n - 1)] + [high]
    totals = [stats_in[i, :, 128:] for i in range(n - 1)] + [total]
    parts = [seen_in[i] for i in range(n - 1)] + [o]
    top = functools.reduce(jnp.maximum, highs)
    scale = [jnp.exp(x - top) for x in highs]
    bottom = functools.reduce(jnp.add, [x * y for x, y in zip(scale, totals)])
    wide = lambda x: jnp.concatenate([x] * (head // 128), -1)
    upper = functools.reduce(jnp.add, [wide(x) * y.astype(jnp.float32) for x, y in zip(scale, parts)])
    out[me] = (upper / wide(bottom)).astype(jnp.bfloat16)

    def result(hop):
        return pltpu.make_async_remote_copy(out.at[me], out.at[me], out_send, out_recv, device_id={"sp": lax.bitwise_xor(me, hop)}, device_id_type=pl.DeviceIdType.MESH)

    @pl.loop(0, n - 1)
    def _(hop):
        result(n - 1 - hop).start()

    pltpu.make_async_copy(seen.at[pl.ds(0, n - 1)], seen.at[pl.ds(0, n - 1)], send_sem.at[0]).wait()
    pltpu.make_async_copy(stats.at[pl.ds(0, n - 1)], stats.at[pl.ds(0, n - 1)], send_sem.at[1]).wait()
    pltpu.make_async_copy(out.at[pl.ds(0, n - 1)], out.at[pl.ds(0, n - 1)], out_send).wait()
    pltpu.make_async_copy(out.at[pl.ds(0, n - 1)], out.at[pl.ds(0, n - 1)], out_recv).wait()


def solution(mesh):
    n = mesh.shape["sp"]

    def step(q, k, v):
        seqs, tokens, heads, head = k.shape
        return pl.pallas_call(
            functools.partial(kernel, n),
            out_shape=jax.ShapeDtypeStruct(q.shape, q.dtype),
            in_specs=[pl.BlockSpec(memory_space=pl.ANY)] * 3,
            out_specs=pl.BlockSpec(memory_space=pltpu.VMEM),
            scratch_shapes=[
                pltpu.VMEM(q.shape, q.dtype),
                pltpu.VMEM((SLOTS, tokens, heads, head), k.dtype),
                pltpu.VMEM((SLOTS, tokens, heads, head), v.dtype),
                pltpu.VMEM((heads, tokens * heads), jnp.float32),
                pltpu.VMEM((heads, tokens * heads), jnp.bfloat16),
                pltpu.VMEM((n, heads, head), jnp.bfloat16),
                pltpu.VMEM((n, heads, 256), jnp.float32),
                pltpu.VMEM((n, heads, head), jnp.bfloat16),
                pltpu.VMEM((n, heads, 256), jnp.float32),
                pltpu.SemaphoreType.DMA,
                pltpu.SemaphoreType.DMA((SLOTS,)),
                pltpu.SemaphoreType.DMA((SLOTS,)),
                pltpu.SemaphoreType.DMA((2,)),
                pltpu.SemaphoreType.DMA((2,)),
                pltpu.SemaphoreType.DMA,
                pltpu.SemaphoreType.DMA,
            ],
            compiler_params=pltpu.CompilerParams(collective_id=0, has_side_effects=True, vmem_limit_bytes=60 * 2**20),
        )(q, k, v)

    return jax.shard_map(
        step,
        mesh=mesh,
        in_specs=(P("dp", None, None), P("dp", "sp", None, None), P("dp", "sp", None, None)),
        out_specs=P("dp", None, None),
        check_vma=False,
    )
```

```python
import functools

import jax
import jax.numpy as jnp
from jax import lax
from jax.experimental import pallas as pl
from jax.experimental.pallas import tpu as pltpu
from jax.sharding import PartitionSpec as P

SLOTS = 8
LAG = 12
LANES = 128
MESH = pl.DeviceIdType.MESH


def kernel(n, q_hbm, k_hbm, v_hbm, out, q, k, v, raw, weights, halves, seen, stats, seen_in, stats_in, merged, merged_stats, q_sem, k_sem, v_sem, send_sem, recv_sem, out_sem):
    me = lax.axis_index("sp")
    chip, core = me // 2, me % 2
    chips = n // 2
    heads, head = q.shape[1:]
    rows = k.shape[1] * heads

    def owner(step):
        if isinstance(step, int) and step >= n - 2:
            return me if step == n - 1 else lax.bitwise_xor(me, 1)
        second = step // (chips - 1)
        other = lax.bitwise_xor(chip, (chips - 1) * (1 + second) - step) * 2 + second
        return other if isinstance(step, int) else jnp.where(step < n - 2, other, jnp.where(step == n - 2, lax.bitwise_xor(me, 1), me))

    def load(hbm, buf, sem, step):
        slot = lax.rem(step, SLOTS)
        return pltpu.make_async_copy(hbm.at[owner(step)], buf.at[slot], sem.at[slot])

    def start(hbm, buf, sem, step):
        load(hbm, buf, sem, step).start()

    def wait(hbm, buf, sem, step):
        load(hbm, buf, sem, step).wait()

    keys, vals = (k_hbm, k, k_sem), (v_hbm, v, v_sem)
    q_copy = pltpu.make_async_copy(q_hbm, q, q_sem)
    q_copy.start()

    @pl.loop(0, SLOTS)
    def _(step):
        start(*keys, step)
        start(*vals, step)

    barrier = pltpu.get_barrier_semaphore()

    @pl.loop(1, n)
    def _(hop):
        pl.semaphore_signal(barrier, inc=1, device_id={"sp": lax.rem(me + hop, n)}, device_id_type=MESH)

    q_copy.wait()
    lane = lax.broadcasted_iota(jnp.int32, (heads, rows), 1)
    own = lane % heads == lax.broadcasted_iota(jnp.int32, (heads, rows), 0)

    def scores(step):
        block = k[lax.rem(step, SLOTS)].reshape(rows, head)
        return lax.dot_general(q[owner(step)], block, (((1,), (1,)), ((), ())), preferred_element_type=jnp.float32)

    def soften(step, s):
        s = jnp.where(own, s * head**-0.5, -jnp.inf)
        high = jnp.max(s, -1, keepdims=True)
        w = jnp.exp(s - high)
        stats[step, :, :LANES] = jnp.broadcast_to(high, (heads, LANES))
        stats[step, :, LANES:] = jnp.broadcast_to(jnp.sum(w, -1, keepdims=True), (heads, LANES))
        return w.astype(jnp.bfloat16)

    def dot(w, block):
        return lax.dot_general(w, block, (((1,), (0,)), ((), ())), preferred_element_type=jnp.float32)

    def values(step, w):
        block = v[lax.rem(step, SLOTS)].reshape(rows, head)
        half = rows // 2
        return dot(w[:, :half], block[:half]) + dot(w[:, half:], block[half:])

    def values_apart(step, w):
        half = v.shape[1] // 2
        for i in range(2):
            halves[i] = dot(w[:, i * rows // 2 : (i + 1) * rows // 2], v[step % SLOTS, i * half : (i + 1) * half].reshape(rows // 2, head))
        return halves[0] + halves[1]

    def send(step):
        to = owner(step)
        slot, group = lax.bitwise_xor(me, to), step // (n - 2)
        for i, (src, dst) in enumerate(((seen, seen_in), (stats, stats_in))):
            pltpu.make_async_remote_copy(
                src.at[step], dst.at[slot], send_sem.at[i], recv_sem.at[group, i], device_id={"sp": to}, device_id_type=MESH
            ).start()

    def put(step, o):
        seen[step] = o.astype(jnp.bfloat16)

    wait(*keys, 0)
    raw[...] = scores(0)
    start(*keys, SLOTS)
    wait(*keys, 1)
    old = raw[...]
    raw[...] = scores(1)
    weights[...] = soften(0, old)
    start(*keys, SLOTS + 1)

    @pl.loop(2, n)
    def _(step):
        wait(*vals, step - 2)
        wait(*keys, step)
        old, w = raw[...], weights[...]
        new = scores(step)
        o = values(step - 2, w)
        weights[...] = soften(step - 1, old)
        raw[...] = new
        put(step - 2, o)

        @pl.when(step - 2 + SLOTS < n)
        def _():
            start(*vals, step - 2 + SLOTS)

        @pl.when(step + SLOTS < n)
        def _():
            start(*keys, step + SLOTS)

        @pl.when(step == LAG)
        def _():
            pl.semaphore_wait(barrier, n - 1)

            @pl.loop(0, LAG - 2)
            def _(earlier):
                send(earlier)

        @pl.when(step >= LAG)
        def _():
            send(step - 2)

    def merge():
        for i, ref in enumerate((seen_in, stats_in)):
            pltpu.make_async_copy(ref.at[pl.ds(2, n - 2)], ref.at[pl.ds(2, n - 2)], recv_sem.at[0, i]).wait()
        top = tree(jnp.maximum, [stats_in[i, :, :LANES] for i in range(2, n)])
        bottoms, uppers = [], []
        for i in range(2, n):
            scale = jnp.exp(stats_in[i, :, :LANES] - top)
            bottoms.append(scale * stats_in[i, :, LANES:])
            uppers.append(wide(scale) * seen_in[i].astype(jnp.float32))
        merged_stats[:, :LANES] = top
        merged_stats[:, LANES:] = tree(jnp.add, bottoms)
        merged[...] = tree(jnp.add, uppers)

    def tree(op, items):
        while len(items) > 1:
            items = [op(*items[i : i + 2]) if i + 1 < len(items) else items[i] for i in range(0, len(items), 2)]
        return items[0]

    def wide(x):
        return jnp.concatenate([x] * (head // LANES), -1)

    before = weights[...]
    w = soften(n - 1, raw[...])
    wait(*vals, n - 2)
    put(n - 2, values(n - 2, before))
    send(n - 2)

    @pl.when(core == 0)
    def _():
        merge()

    wait(*vals, n - 1)
    halves[0] = values_apart(n - 1, w)

    @pl.when(core == 1)
    def _():
        merge()

    for i, ref in enumerate((seen_in, stats_in)):
        pltpu.make_async_copy(ref.at[1], ref.at[1], recv_sem.at[1, i]).wait()
    highs = [stats[n - 1, :, :LANES], stats_in[1, :, :LANES], merged_stats[:, :LANES]]
    totals = [stats[n - 1, :, LANES:], stats_in[1, :, LANES:], merged_stats[:, LANES:]]
    parts = [halves[0], seen_in[1].astype(jnp.float32), merged[...]]
    top = tree(jnp.maximum, highs)
    scales = [jnp.exp(x - top) for x in highs]
    bottom = tree(jnp.add, [x * y for x, y in zip(scales, totals)])
    upper = tree(jnp.add, [wide(x) * y for x, y in zip(scales, parts)])
    out[me] = (upper / wide(bottom)).astype(jnp.bfloat16)

    @pl.loop(0, n - 1)
    def _(i):
        to = i + (i >= me).astype(jnp.int32)
        pltpu.make_async_remote_copy(out.at[me], out.at[me], out_sem.at[0], out_sem.at[1], device_id={"sp": to}, device_id_type=MESH).start()

    for ref, sem in ((seen, send_sem.at[0]), (stats, send_sem.at[1]), (out, out_sem.at[0]), (out, out_sem.at[1])):
        pltpu.make_async_copy(ref.at[pl.ds(0, n - 1)], ref.at[pl.ds(0, n - 1)], sem).wait()


def solution(mesh):
    n = mesh.shape["sp"]

    def step(q, k, v):
        seqs, tokens, heads, head = k.shape
        assert seqs == n
        return pl.pallas_call(
            functools.partial(kernel, n),
            out_shape=pltpu.VMEM(q.shape, q.dtype),
            in_specs=[pl.BlockSpec(memory_space=pltpu.HBM)] * 3,
            out_specs=pl.BlockSpec(memory_space=pltpu.VMEM),
            scratch_shapes=[
                pltpu.VMEM(q.shape, q.dtype),
                pltpu.VMEM((SLOTS, tokens, heads, head), k.dtype),
                pltpu.VMEM((SLOTS, tokens, heads, head), v.dtype),
                pltpu.VMEM((heads, tokens * heads), jnp.float32),
                pltpu.VMEM((heads, tokens * heads), jnp.bfloat16),
                pltpu.VMEM((2, heads, head), jnp.float32),
                pltpu.VMEM((n, heads, head), jnp.bfloat16),
                pltpu.VMEM((n, heads, 2 * LANES), jnp.float32),
                pltpu.VMEM((n, heads, head), jnp.bfloat16),
                pltpu.VMEM((n, heads, 2 * LANES), jnp.float32),
                pltpu.VMEM((heads, head), jnp.float32),
                pltpu.VMEM((heads, 2 * LANES), jnp.float32),
                pltpu.SemaphoreType.DMA,
                pltpu.SemaphoreType.DMA((SLOTS,)),
                pltpu.SemaphoreType.DMA((SLOTS,)),
                pltpu.SemaphoreType.DMA((2,)),
                pltpu.SemaphoreType.DMA((2, 2)),
                pltpu.SemaphoreType.DMA((2,)),
            ],
            compiler_params=pltpu.CompilerParams(collective_id=0, has_side_effects=True, vmem_limit_bytes=67043328 - 192 * 1024),
        )(q, k, v)

    return jax.shard_map(
        step,
        mesh=mesh,
        in_specs=(P("dp", None, None), P("dp", "sp", None, None), P("dp", "sp", None, None)),
        out_specs=P("dp", None, None),
        check_vma=False,
    )
```

```python
import functools

import jax
import jax.numpy as jnp
from jax import lax
from jax.experimental import pallas as pl
from jax.experimental.pallas import tpu as pltpu
from jax.sharding import PartitionSpec as P

SLOTS = 8
LAG = 12
LANES = 128
MESH = pl.DeviceIdType.MESH


def kernel(n, q_hbm, k_hbm, v_hbm, out, q, k, v, raw, weights, halves, last, seen, stats, seen_in, stats_in, merged, merged_stats, q_sem, k_sem, v_sem, send_sem, recv_sem, out_sem):
    me = lax.axis_index("sp")
    chip, core = me // 2, me % 2
    chips = n // 2
    heads, head = q.shape[1:]
    rows = k.shape[1] * heads

    def owner(step):
        if isinstance(step, int) and step >= n - 2:
            return me if step == n - 1 else lax.bitwise_xor(me, 1)
        second = step // (chips - 1)
        other = lax.bitwise_xor(chip, (chips - 1) * (1 + second) - step) * 2 + second
        return other if isinstance(step, int) else jnp.where(step < n - 2, other, jnp.where(step == n - 2, lax.bitwise_xor(me, 1), me))

    def load(hbm, buf, sem, step):
        slot = lax.rem(step, SLOTS)
        return pltpu.make_async_copy(hbm.at[owner(step)], buf.at[slot], sem.at[slot])

    def start(hbm, buf, sem, step):
        load(hbm, buf, sem, step).start()

    def wait(hbm, buf, sem, step):
        load(hbm, buf, sem, step).wait()

    keys, vals = (k_hbm, k, k_sem), (v_hbm, v, v_sem)
    q_copy = pltpu.make_async_copy(q_hbm, q, q_sem)
    q_copy.start()

    @pl.loop(0, SLOTS)
    def _(step):
        start(*keys, step)
        start(*vals, step)

    barrier = pltpu.get_barrier_semaphore()

    @pl.loop(1, n)
    def _(hop):
        pl.semaphore_signal(barrier, inc=1, device_id={"sp": lax.rem(me + hop, n)}, device_id_type=MESH)

    q_copy.wait()
    lane = lax.broadcasted_iota(jnp.int32, (heads, rows), 1)
    own = lane % heads == lax.broadcasted_iota(jnp.int32, (heads, rows), 0)

    def scores(step):
        block = k[lax.rem(step, SLOTS)].reshape(rows, head)
        return lax.dot_general(q[owner(step)], block, (((1,), (1,)), ((), ())), preferred_element_type=jnp.float32)

    def soften(step, s):
        s = jnp.where(own, s * head**-0.5, -jnp.inf)
        high = jnp.max(s, -1, keepdims=True)
        w = jnp.exp(s - high)
        stats[step, :, :LANES] = jnp.broadcast_to(high, (heads, LANES))
        stats[step, :, LANES:] = jnp.broadcast_to(jnp.sum(w, -1, keepdims=True), (heads, LANES))
        return w.astype(jnp.bfloat16)

    def dot(w, block):
        return lax.dot_general(w, block, (((1,), (0,)), ((), ())), preferred_element_type=jnp.float32)

    def values(step, w):
        block = v[lax.rem(step, SLOTS)].reshape(rows, head)
        half = rows // 2
        return dot(w[:, :half], block[:half]) + dot(w[:, half:], block[half:])

    def values_apart(step, w):
        half = v.shape[1] // 2
        for i in range(2):
            halves[i] = dot(w[:, i * rows // 2 : (i + 1) * rows // 2], v[step % SLOTS, i * half : (i + 1) * half].reshape(rows // 2, head))
        return halves[0] + halves[1]

    def send(step):
        to = owner(step)
        slot, group = lax.bitwise_xor(me, to), step // (n - 2)
        for i, (src, dst) in enumerate(((seen, seen_in), (stats, stats_in))):
            pltpu.make_async_remote_copy(
                src.at[step], dst.at[slot], send_sem.at[i], recv_sem.at[group, i], device_id={"sp": to}, device_id_type=MESH
            ).start()

    def put(step, o):
        seen[step] = o.astype(jnp.bfloat16)

    def merge():
        for i, ref in enumerate((seen_in, stats_in)):
            pltpu.make_async_copy(ref.at[pl.ds(2, n - 2)], ref.at[pl.ds(2, n - 2)], recv_sem.at[0, i]).wait()
        top = tree(jnp.maximum, [stats_in[i, :, :LANES] for i in range(2, n)])
        bottoms, uppers = [], []
        for i in range(2, n):
            scale = jnp.exp(stats_in[i, :, :LANES] - top)
            bottoms.append(scale * stats_in[i, :, LANES:])
            uppers.append(wide(scale) * seen_in[i].astype(jnp.float32))
        merged_stats[:, :LANES] = top
        merged_stats[:, LANES:] = tree(jnp.add, bottoms)
        merged[...] = tree(jnp.add, uppers)

    def tree(op, items):
        while len(items) > 1:
            items = [op(*items[i : i + 2]) if i + 1 < len(items) else items[i] for i in range(0, len(items), 2)]
        return items[0]

    def wide(x):
        return jnp.concatenate([x] * (head // LANES), -1)

    wait(*keys, 0)
    raw[...] = scores(0)
    start(*keys, SLOTS)
    wait(*keys, 1)
    old = raw[...]
    raw[...] = scores(1)
    weights[...] = soften(0, old)
    start(*keys, SLOTS + 1)

    @pl.loop(2, n - 2)
    def _(step):
        wait(*vals, step - 2)
        wait(*keys, step)
        old, w = raw[...], weights[...]
        new = scores(step)
        o = values(step - 2, w)
        weights[...] = soften(step - 1, old)
        raw[...] = new
        put(step - 2, o)

        @pl.when(step - 2 + SLOTS < n)
        def _():
            start(*vals, step - 2 + SLOTS)

        @pl.when(step + SLOTS < n - 2)
        def _():
            start(*keys, step + SLOTS)

        @pl.when(step - 2 + SLOTS == n - 3)
        def _():
            start(*keys, n - 2)
            start(*keys, n - 1)

        @pl.when(step == LAG)
        def _():
            pl.semaphore_wait(barrier, n - 1)

            @pl.loop(0, LAG - 2)
            def _(earlier):
                send(earlier)

        @pl.when(step >= LAG)
        def _():
            send(step - 2)

        @pl.when((step == n - 6) & (core == 0))
        def _():
            merge()

    def block(f):
        @pl.loop(0, 1 + me // n)
        def _(_):
            f()

    @block
    def _():
        w = soften(n - 3, raw[...])
        wait(*vals, n - 4)
        put(n - 4, values_apart(n - 4, weights[...]))
        weights[...] = w
        send(n - 4)

    @block
    def _():
        wait(*vals, n - 3)
        put(n - 3, values_apart(n - 3, weights[...]))
        send(n - 3)

    @block
    def _():
        wait(*keys, n - 2)
        raw[...] = scores(n - 2)

    @block
    def _():
        wait(*keys, n - 1)
        old = raw[...]
        raw[...] = scores(n - 1)
        weights[...] = soften(n - 2, old)

    @block
    def _():
        wait(*vals, n - 2)
        put(n - 2, values_apart(n - 2, weights[...]))
        weights[...] = soften(n - 1, raw[...])
        send(n - 2)

    @block
    def _():
        wait(*vals, n - 1)
        last[...] = values_apart(n - 1, weights[...])

    @pl.when(core == 1)
    def _():
        merge()

    for i, ref in enumerate((seen_in, stats_in)):
        pltpu.make_async_copy(ref.at[1], ref.at[1], recv_sem.at[1, i]).wait()
    highs = [stats[n - 1, :, :LANES], stats_in[1, :, :LANES], merged_stats[:, :LANES]]
    totals = [stats[n - 1, :, LANES:], stats_in[1, :, LANES:], merged_stats[:, LANES:]]
    parts = [last[...], seen_in[1].astype(jnp.float32), merged[...]]
    top = tree(jnp.maximum, highs)
    scales = [jnp.exp(x - top) for x in highs]
    bottom = tree(jnp.add, [x * y for x, y in zip(scales, totals)])
    upper = tree(jnp.add, [wide(x) * y for x, y in zip(scales, parts)])
    out[me] = (upper / wide(bottom)).astype(jnp.bfloat16)

    @pl.loop(0, n - 1)
    def _(i):
        to = i + (i >= me).astype(jnp.int32)
        pltpu.make_async_remote_copy(out.at[me], out.at[me], out_sem.at[0], out_sem.at[1], device_id={"sp": to}, device_id_type=MESH).start()

    for ref, sem in ((seen, send_sem.at[0]), (stats, send_sem.at[1]), (out, out_sem.at[0]), (out, out_sem.at[1])):
        pltpu.make_async_copy(ref.at[pl.ds(0, n - 1)], ref.at[pl.ds(0, n - 1)], sem).wait()


def solution(mesh):
    n = mesh.shape["sp"]

    def step(q, k, v):
        seqs, tokens, heads, head = k.shape
        assert seqs == n
        return pl.pallas_call(
            functools.partial(kernel, n),
            out_shape=pltpu.VMEM(q.shape, q.dtype),
            in_specs=[pl.BlockSpec(memory_space=pltpu.HBM)] * 3,
            out_specs=pl.BlockSpec(memory_space=pltpu.VMEM),
            scratch_shapes=[
                pltpu.VMEM(q.shape, q.dtype),
                pltpu.VMEM((SLOTS, tokens, heads, head), k.dtype),
                pltpu.VMEM((SLOTS, tokens, heads, head), v.dtype),
                pltpu.VMEM((heads, tokens * heads), jnp.float32),
                pltpu.VMEM((heads, tokens * heads), jnp.bfloat16),
                pltpu.VMEM((2, heads, head), jnp.float32),
                pltpu.VMEM((heads, head), jnp.float32),
                pltpu.VMEM((n, heads, head), jnp.bfloat16),
                pltpu.VMEM((n, heads, 2 * LANES), jnp.float32),
                pltpu.VMEM((n, heads, head), jnp.bfloat16),
                pltpu.VMEM((n, heads, 2 * LANES), jnp.float32),
                pltpu.VMEM((heads, head), jnp.float32),
                pltpu.VMEM((heads, 2 * LANES), jnp.float32),
                pltpu.SemaphoreType.DMA,
                pltpu.SemaphoreType.DMA((SLOTS,)),
                pltpu.SemaphoreType.DMA((SLOTS,)),
                pltpu.SemaphoreType.DMA((2,)),
                pltpu.SemaphoreType.DMA((2, 2)),
                pltpu.SemaphoreType.DMA((2,)),
            ],
            compiler_params=pltpu.CompilerParams(collective_id=0, has_side_effects=True, vmem_limit_bytes=67043328 - 192 * 1024),
        )(q, k, v)

    return jax.shard_map(
        step,
        mesh=mesh,
        in_specs=(P("dp", None, None), P("dp", "sp", None, None), P("dp", "sp", None, None)),
        out_specs=P("dp", None, None),
        check_vma=False,
    )
```

```python
import functools

import jax
import jax.numpy as jnp
from jax import lax
from jax.experimental import pallas as pl
from jax.experimental.pallas import tpu as pltpu
from jax.sharding import PartitionSpec as P

SLOTS = 8
LAG = 13
BEHIND = 4
LANES = 128
MESH = pl.DeviceIdType.MESH


def kernel(n, q_hbm, k_hbm, v_hbm, out, q, k, v, raw, weights, halves, last, seen, stats, seen_in, stats_in, merged, merged_stats, q_sem, k_sem, v_sem, send_sem, recv_sem, out_sem):
    me = lax.axis_index("sp")
    chip, core = me // 2, me % 2
    chips = n // 2
    heads, head = q.shape[1:]
    rows = k.shape[1] * heads

    near, far = chip == 0, chip == chips - 1

    def work(step):
        step = jnp.asarray(step, jnp.int32)
        last_two, skips = step - (n - 2), jnp.where(near, 0, 1)
        turn = step - jnp.where(far, 0, 2)
        second = (turn >= chips - 1 - skips).astype(jnp.int32)
        mask = chips - 1 - (turn - second * (chips - 1 - skips))
        mask = mask - jnp.where(near, 0, (mask <= chip).astype(jnp.int32))
        to_far = chips - 1 - chip
        swaps = jnp.logical_not(far) & (to_far < 4)
        mask = jnp.where(swaps & (mask == chips - 1), to_far, jnp.where(swaps & (mask == to_far), chips - 1, mask))
        seq = lax.bitwise_xor(chip, mask) * 2 + second
        seq = jnp.where((last_two >= 0) & jnp.logical_not(near), lax.bitwise_xor(me, 1 - last_two), seq)
        end = lax.bitwise_xor(me, (step < n - 2).astype(jnp.int32)) - jnp.where((step == n - 3) | (step == n - 2), n - 2, 0)
        return jnp.where(far & (step >= n - 4), end, jnp.where(jnp.logical_not(far) & (step < 2), step, seq))

    early = (core == 0) & jnp.logical_not(near)

    def owner(seq):
        return seq + jnp.where(seq < 2, n - 2, 0)

    def load(hbm, buf, sem, step):
        slot = lax.rem(step, SLOTS)
        return pltpu.make_async_copy(hbm.at[work(step)], buf.at[slot], sem.at[slot])

    def start(hbm, buf, sem, step):
        load(hbm, buf, sem, step).start()

    def wait(hbm, buf, sem, step):
        load(hbm, buf, sem, step).wait()

    keys, vals = (k_hbm, k, k_sem), (v_hbm, v, v_sem)
    q_copy = pltpu.make_async_copy(q_hbm, q, q_sem)
    q_copy.start()

    @pl.loop(0, BEHIND)
    def _(step):
        start(*keys, step)

    @pl.loop(0, SLOTS)
    def _(step):
        start(*vals, step)

        @pl.when(step + BEHIND < SLOTS)
        def _():
            start(*keys, step + BEHIND)

    barrier = pltpu.get_barrier_semaphore()

    @pl.loop(1, n)
    def _(hop):
        pl.semaphore_signal(barrier, inc=1, device_id={"sp": lax.rem(me + hop, n)}, device_id_type=MESH)

    q_copy.wait()
    lane = lax.broadcasted_iota(jnp.int32, (heads, rows), 1)
    own = lane % heads == lax.broadcasted_iota(jnp.int32, (heads, rows), 0)

    def scores(step):
        block = k[lax.rem(step, SLOTS)].reshape(rows, head)
        return lax.dot_general(q[work(step)], block, (((1,), (1,)), ((), ())), preferred_element_type=jnp.float32)

    def soften(step, s):
        s = jnp.where(own, s * head**-0.5, -jnp.inf)
        high = jnp.max(s, -1, keepdims=True)
        w = jnp.exp(s - high)
        stats[step, :, :LANES] = jnp.broadcast_to(high, (heads, LANES))
        stats[step, :, LANES:] = jnp.broadcast_to(jnp.sum(w, -1, keepdims=True), (heads, LANES))
        return w.astype(jnp.bfloat16)

    def dot(w, block):
        return lax.dot_general(w, block, (((1,), (0,)), ((), ())), preferred_element_type=jnp.float32)

    def values(step, w):
        block = v[lax.rem(step, SLOTS)].reshape(rows, head)
        half = rows // 2
        return dot(w[:, :half], block[:half]) + dot(w[:, half:], block[half:])

    def values_apart(i, step, w):
        half = v.shape[1] // 2
        for part in range(2):
            halves[i, part] = dot(w[:, part * rows // 2 : (part + 1) * rows // 2], v[step % SLOTS, part * half : (part + 1) * half].reshape(rows // 2, head))
        return halves[i, 0] + halves[i, 1]

    def send(step):
        seq = work(step)
        to = owner(seq)
        which = lax.bitwise_xor(me, to)
        extra = (seq < 2).astype(jnp.int32)

        @pl.when(which > 0)
        def _():
            for i, (src, dst) in enumerate(((seen, seen_in), (stats, stats_in))):
                pltpu.make_async_remote_copy(
                    src.at[step],
                    dst.at[extra, which],
                    send_sem.at[i],
                    recv_sem.at[extra, (which == 1).astype(jnp.int32), i],
                    device_id={"sp": to},
                    device_id_type=MESH,
                ).start()

    def put(step, o):
        seen[step] = o.astype(jnp.bfloat16)

    def merge(extra):
        for i, ref in enumerate((seen_in, stats_in)):
            pltpu.make_async_copy(ref.at[extra, pl.ds(2, n - 2)], ref.at[extra, pl.ds(2, n - 2)], recv_sem.at[extra, 0, i]).wait()
        top = tree(jnp.maximum, [stats_in[extra, i, :, :LANES] for i in range(2, n)])
        bottoms, uppers = [], []
        for i in range(2, n):
            scale = jnp.exp(stats_in[extra, i, :, :LANES] - top)
            bottoms.append(scale * stats_in[extra, i, :, LANES:])
            uppers.append(wide(scale) * seen_in[extra, i].astype(jnp.float32))
        merged_stats[extra, :, :LANES] = top
        merged_stats[extra, :, LANES:] = tree(jnp.add, bottoms)
        merged[extra] = tree(jnp.add, uppers)

    def tree(op, items):
        while len(items) > 1:
            items = [op(*items[i : i + 2]) if i + 1 < len(items) else items[i] for i in range(0, len(items), 2)]
        return items[0]

    def wide(x):
        return jnp.concatenate([x] * (head // LANES), -1)

    def keep(step, w):
        weights[lax.rem(step, BEHIND)] = w

    @pl.loop(0, BEHIND)
    def _(step):
        wait(*keys, step)
        old = raw[...]
        raw[...] = scores(step)

        @pl.when(step > 0)
        def _():
            keep(step - 1, soften(step - 1, old))

        start(*keys, step + SLOTS)

    @pl.loop(BEHIND, n)
    def _(step):
        wait(*vals, step - BEHIND)
        wait(*keys, step)
        old, w = raw[...], weights[lax.rem(step, BEHIND)]
        new = scores(step)
        o = values(step - BEHIND, w)
        keep(step - 1, soften(step - 1, old))
        raw[...] = new
        put(step - BEHIND, o)

        @pl.when(step - BEHIND + SLOTS < n)
        def _():
            start(*vals, step - BEHIND + SLOTS)

        @pl.when(step + SLOTS < n)
        def _():
            start(*keys, step + SLOTS)

        @pl.when(step == LAG)
        def _():
            pl.semaphore_wait(barrier, n - 1)

            @pl.loop(0, LAG - BEHIND)
            def _(earlier):
                send(earlier)

        @pl.when(step >= LAG)
        def _():
            send(step - BEHIND)

        @pl.when((step == n - 4) & far)
        def _():
            merge(1)

        @pl.when((step == n - 4) & early)
        def _():
            merge(0)

    def block(f):
        @pl.loop(0, 1 + me // n)
        def _(_):
            f()

    def finish(step):
        wait(*vals, step)
        o = values_apart(0, step, weights[step % BEHIND])
        put(step, o)
        if step >= n - 2:
            last[n - 1 - step] = o
        send(step)

    @block
    def _():
        keep(n - 1, soften(n - 1, raw[...]))
        finish(n - BEHIND)

    for step in range(n - BEHIND + 1, n):
        block(functools.partial(finish, step))

    @pl.when((core == 1) & jnp.logical_not(near))
    def _():
        merge(0)

    def combine(extra, seq):
        for i, ref in enumerate((seen_in, stats_in)):
            pltpu.make_async_copy(ref.at[extra, 1], ref.at[extra, 1], recv_sem.at[extra, 1, i]).wait()
        mine = stats[n - 1 - extra]
        both = [mine, stats_in[extra, 1], merged_stats[extra]]
        highs, totals = [x[:, :LANES] for x in both], [x[:, LANES:] for x in both]
        parts = [last[extra], seen_in[extra, 1].astype(jnp.float32), merged[extra]]
        top = tree(jnp.maximum, highs)
        scales = [jnp.exp(x - top) for x in highs]
        bottom = tree(jnp.add, [x * y for x, y in zip(scales, totals)])
        upper = tree(jnp.add, [wide(x) * y for x, y in zip(scales, parts)])
        out[seq] = (upper / wide(bottom)).astype(jnp.bfloat16)

    def share(seq, to):
        pltpu.make_async_remote_copy(out.at[seq], out.at[seq], out_sem.at[0], out_sem.at[1], device_id={"sp": to}, device_id_type=MESH).start()

    @pl.when(far)
    def _():
        combine(1, core)
        share(core, 0)
        share(core, 1)

    @pl.when(jnp.logical_not(near))
    def _():
        combine(0, me)
        share(me, 0)
        share(me, 1)

        @pl.loop(1, n)
        def _(i):
            to = lax.bitwise_xor(me, n - i)

            @pl.when(to >= 2)
            def _():
                share(me, to)

                @pl.when(far)
                def _():
                    share(core, to)

    middle = jnp.logical_not(near | far)

    def ended(ref, sem, *counts):
        for chips_of, count in zip((near, far, middle), counts):
            if count:
                block = ref.at[pl.ds(0, count)] if count <= n else seen_in.at[:, pl.ds(0, count // 2)]
                pl.when(chips_of)(pltpu.make_async_copy(block, block, sem).wait)

    ended(seen, send_sem.at[0], n, n - 2, n - 1)
    ended(stats, send_sem.at[1], n, n - 2, n - 1)
    ended(out, out_sem.at[0], 0, 2 * n - 2, n - 1)
    ended(out, out_sem.at[1], n, n - 2, n - 1)


def solution(mesh):
    n = mesh.shape["sp"]

    def step(q, k, v):
        seqs, tokens, heads, head = k.shape
        assert seqs == n
        return pl.pallas_call(
            functools.partial(kernel, n),
            out_shape=pltpu.VMEM(q.shape, q.dtype),
            in_specs=[pl.BlockSpec(memory_space=pltpu.HBM)] * 3,
            out_specs=pl.BlockSpec(memory_space=pltpu.VMEM),
            scratch_shapes=[
                pltpu.VMEM(q.shape, q.dtype),
                pltpu.VMEM((SLOTS, tokens, heads, head), k.dtype),
                pltpu.VMEM((SLOTS, tokens, heads, head), v.dtype),
                pltpu.VMEM((heads, tokens * heads), jnp.float32),
                pltpu.VMEM((BEHIND, heads, tokens * heads), jnp.bfloat16),
                pltpu.VMEM((2, 2, heads, head), jnp.float32),
                pltpu.VMEM((2, heads, head), jnp.float32),
                pltpu.VMEM((n, heads, head), jnp.bfloat16),
                pltpu.VMEM((n, heads, 2 * LANES), jnp.float32),
                pltpu.VMEM((2, n, heads, head), jnp.bfloat16),
                pltpu.VMEM((2, n, heads, 2 * LANES), jnp.float32),
                pltpu.VMEM((2, heads, head), jnp.float32),
                pltpu.VMEM((2, heads, 2 * LANES), jnp.float32),
                pltpu.SemaphoreType.DMA,
                pltpu.SemaphoreType.DMA((SLOTS,)),
                pltpu.SemaphoreType.DMA((SLOTS,)),
                pltpu.SemaphoreType.DMA((2,)),
                pltpu.SemaphoreType.DMA((2, 2, 2)),
                pltpu.SemaphoreType.DMA((2,)),
            ],
            compiler_params=pltpu.CompilerParams(collective_id=0, has_side_effects=True, vmem_limit_bytes=67043328 - 192 * 1024),
        )(q, k, v)

    return jax.shard_map(
        step,
        mesh=mesh,
        in_specs=(P("dp", None, None), P("dp", "sp", None, None), P("dp", "sp", None, None)),
        out_specs=P("dp", None, None),
        check_vma=False,
    )
```

```python
import functools

import jax
import jax.numpy as jnp
from jax import lax
from jax.experimental import pallas as pl
from jax.experimental.pallas import tpu as pltpu
from jax.sharding import PartitionSpec as P

SLOTS = 8
LAG = 13
BEHIND = 4
LANES = 128
MESH = pl.DeviceIdType.MESH


def kernel(n, q_hbm, k_hbm, v_hbm, out, q, k, v, raw, weights, halves, last, seen, stats, seen_in, stats_in, merged, merged_stats, q_sem, k_sem, v_sem, send_sem, recv_sem, out_sem):
    me = lax.axis_index("sp")
    chip, core = me // 2, me % 2
    chips = n // 2
    heads, head = q.shape[1:]
    rows = k.shape[1] * heads

    near, far = chip == 0, chip == chips - 1

    def work(step):
        step = jnp.asarray(step, jnp.int32)
        last_two, skips = step - (n - 2), jnp.where(near, 0, 1)
        turn = step - jnp.where(far, 0, 2)
        second = (turn >= chips - 1 - skips).astype(jnp.int32)
        mask = chips - 1 - (turn - second * (chips - 1 - skips))
        mask = mask - jnp.where(near, 0, (mask <= chip).astype(jnp.int32))
        to_far = chips - 1 - chip
        swaps = jnp.logical_not(far) & (to_far < 4)
        mask = jnp.where(swaps & (mask == chips - 1), to_far, jnp.where(swaps & (mask == to_far), chips - 1, mask))
        seq = lax.bitwise_xor(chip, mask) * 2 + second
        seq = jnp.where((last_two >= 0) & jnp.logical_not(near), lax.bitwise_xor(me, 1 - last_two), seq)
        end = lax.bitwise_xor(me, (step < n - 2).astype(jnp.int32)) - jnp.where((step == n - 3) | (step == n - 2), n - 2, 0)
        return jnp.where(far & (step >= n - 4), end, jnp.where(jnp.logical_not(far) & (step < 2), step, seq))

    early = (core == 0) & jnp.logical_not(near)

    def owner(seq):
        return seq + jnp.where(seq < 2, n - 2, 0)

    def load(hbm, buf, sem, step):
        slot = lax.rem(step, SLOTS)
        return pltpu.make_async_copy(hbm.at[work(step)], buf.at[slot], sem.at[slot])

    def start(hbm, buf, sem, step):
        load(hbm, buf, sem, step).start()

    def wait(hbm, buf, sem, step):
        load(hbm, buf, sem, step).wait()

    keys, vals = (k_hbm, k, k_sem), (v_hbm, v, v_sem)
    q_copy = pltpu.make_async_copy(q_hbm, q, q_sem)
    q_copy.start()

    @pl.loop(0, BEHIND)
    def _(step):
        start(*keys, step)

    @pl.loop(0, SLOTS)
    def _(step):
        start(*vals, step)

        @pl.when(step + BEHIND < SLOTS)
        def _():
            start(*keys, step + BEHIND)

    barrier = pltpu.get_barrier_semaphore()

    @pl.loop(1, n)
    def _(hop):
        pl.semaphore_signal(barrier, inc=1, device_id={"sp": lax.rem(me + hop, n)}, device_id_type=MESH)

    q_copy.wait()
    lane = lax.broadcasted_iota(jnp.int32, (heads, rows), 1)
    own = lane % heads == lax.broadcasted_iota(jnp.int32, (heads, rows), 0)

    def scores(step):
        block = k[lax.rem(step, SLOTS)].reshape(rows, head)
        return lax.dot_general(q[work(step)], block, (((1,), (1,)), ((), ())), preferred_element_type=jnp.float32)

    def soften(step, s):
        s = jnp.where(own, s * head**-0.5, -jnp.inf)
        high = jnp.max(s, -1, keepdims=True)
        w = jnp.exp(s - high)
        stats[step, :, :LANES] = jnp.broadcast_to(high, (heads, LANES))
        stats[step, :, LANES:] = jnp.broadcast_to(jnp.sum(w, -1, keepdims=True), (heads, LANES))
        return w.astype(jnp.bfloat16)

    def dot(w, block):
        return lax.dot_general(w, block, (((1,), (0,)), ((), ())), preferred_element_type=jnp.float32)

    def values(step, w):
        block = v[lax.rem(step, SLOTS)].reshape(rows, head)
        half = rows // 2
        return dot(w[:, :half], block[:half]) + dot(w[:, half:], block[half:])

    def values_apart(i, step, w):
        half = v.shape[1] // 2
        for part in range(2):
            halves[i, part] = dot(w[:, part * rows // 2 : (part + 1) * rows // 2], v[step % SLOTS, part * half : (part + 1) * half].reshape(rows // 2, head))
        return halves[i, 0] + halves[i, 1]

    def send(step):
        seq = work(step)
        to = owner(seq)
        which = lax.bitwise_xor(me, to)
        extra = (seq < 2).astype(jnp.int32)

        @pl.when(which > 0)
        def _():
            for i, (src, dst) in enumerate(((seen, seen_in), (stats, stats_in))):
                pltpu.make_async_remote_copy(
                    src.at[step],
                    dst.at[extra, which],
                    send_sem.at[i],
                    recv_sem.at[extra, (which == 1).astype(jnp.int32), i],
                    device_id={"sp": to},
                    device_id_type=MESH,
                ).start()

    def put(step, o):
        seen[step] = o.astype(jnp.bfloat16)

    def merge(extra):
        for i, ref in enumerate((seen_in, stats_in)):
            pltpu.make_async_copy(ref.at[extra, pl.ds(2, n - 2)], ref.at[extra, pl.ds(2, n - 2)], recv_sem.at[extra, 0, i]).wait()
        top = tree(jnp.maximum, [stats_in[extra, i, :, :LANES] for i in range(2, n)])
        bottoms, uppers = [], []
        for i in range(2, n):
            scale = jnp.exp(stats_in[extra, i, :, :LANES] - top)
            bottoms.append(scale * stats_in[extra, i, :, LANES:])
            uppers.append(wide(scale) * seen_in[extra, i].astype(jnp.float32))
        merged_stats[extra, :, :LANES] = top
        merged_stats[extra, :, LANES:] = tree(jnp.add, bottoms)
        merged[extra] = tree(jnp.add, uppers)

    def tree(op, items):
        while len(items) > 1:
            items = [op(*items[i : i + 2]) if i + 1 < len(items) else items[i] for i in range(0, len(items), 2)]
        return items[0]

    def wide(x):
        return jnp.concatenate([x] * (head // LANES), -1)

    def keep(step, w):
        weights[lax.rem(step, BEHIND)] = w

    @pl.loop(0, BEHIND)
    def _(step):
        wait(*keys, step)
        old = raw[...]
        raw[...] = scores(step)

        @pl.when(step > 0)
        def _():
            keep(step - 1, soften(step - 1, old))

        start(*keys, step + SLOTS)

    @pl.loop(BEHIND, n)
    def _(step):
        wait(*vals, step - BEHIND)
        wait(*keys, step)
        old, w = raw[...], weights[lax.rem(step, BEHIND)]
        new = scores(step)
        o = values(step - BEHIND, w)
        keep(step - 1, soften(step - 1, old))
        raw[...] = new
        put(step - BEHIND, o)

        @pl.when(step - BEHIND + SLOTS < n)
        def _():
            start(*vals, step - BEHIND + SLOTS)

        @pl.when(step + SLOTS < n)
        def _():
            start(*keys, step + SLOTS)

        @pl.when(step == LAG)
        def _():
            pl.semaphore_wait(barrier, n - 1)

            @pl.loop(0, LAG - BEHIND)
            def _(earlier):
                send(earlier)

        @pl.when(step >= LAG)
        def _():
            send(step - BEHIND)

        @pl.when((step == n - 4) & far)
        def _():
            merge(1)

        @pl.when((step == n - 4) & early)
        def _():
            merge(0)

    def block(f):
        @pl.loop(0, 1 + me // n)
        def _(_):
            f()

    def finish(step):
        wait(*vals, step)
        o = values_apart(0, step, weights[step % BEHIND])
        put(step, o)
        if step >= n - 2:
            last[n - 1 - step] = o
        send(step)

    @block
    def _():
        keep(n - 1, soften(n - 1, raw[...]))
        finish(n - BEHIND)

    for step in range(n - BEHIND + 1, n):
        block(functools.partial(finish, step))

    @pl.when((core == 1) & jnp.logical_not(near))
    def _():
        merge(0)

    def combine(extra, seq):
        for i, ref in enumerate((seen_in, stats_in)):
            pltpu.make_async_copy(ref.at[extra, 1], ref.at[extra, 1], recv_sem.at[extra, 1, i]).wait()
        mine = stats[n - 1 - extra]
        both = [mine, stats_in[extra, 1], merged_stats[extra]]
        highs, totals = [x[:, :LANES] for x in both], [x[:, LANES:] for x in both]
        parts = [last[extra], seen_in[extra, 1].astype(jnp.float32), merged[extra]]
        top = tree(jnp.maximum, highs)
        scales = [jnp.exp(x - top) for x in highs]
        bottom = tree(jnp.add, [x * y for x, y in zip(scales, totals)])
        upper = tree(jnp.add, [wide(x) * y for x, y in zip(scales, parts)])
        out[seq] = (upper / wide(bottom)).astype(jnp.bfloat16)

    def share(seq, to):
        pltpu.make_async_remote_copy(out.at[seq], out.at[seq], out_sem.at[0], out_sem.at[1], device_id={"sp": to}, device_id_type=MESH).start()

    @pl.when(far)
    def _():
        combine(1, core)
        share(core, 0)
        share(core, 1)

    @pl.when(jnp.logical_not(near))
    def _():
        combine(0, me)
        share(me, 0)
        share(me, 1)

        @pl.loop(0, n)
        def _(i):
            to = lax.bitwise_xor(me, jnp.where(far, n - 1 - i, lax.rem(i + n // 4, n)))

            @pl.when((to >= 2) & (to != me))
            def _():
                share(me, to)

                @pl.when(far)
                def _():
                    share(core, to)

    middle = jnp.logical_not(near | far)

    def ended(ref, sem, *counts):
        for chips_of, count in zip((near, far, middle), counts):
            if count:
                block = ref.at[pl.ds(0, count)] if count <= n else seen_in.at[:, pl.ds(0, count // 2)]
                pl.when(chips_of)(pltpu.make_async_copy(block, block, sem).wait)

    ended(seen, send_sem.at[0], n, n - 2, n - 1)
    ended(stats, send_sem.at[1], n, n - 2, n - 1)
    ended(out, out_sem.at[0], 0, 2 * n - 2, n - 1)
    ended(out, out_sem.at[1], n, n - 2, n - 1)


def solution(mesh):
    n = mesh.shape["sp"]

    def step(q, k, v):
        seqs, tokens, heads, head = k.shape
        assert seqs == n
        return pl.pallas_call(
            functools.partial(kernel, n),
            out_shape=pltpu.VMEM(q.shape, q.dtype),
            in_specs=[pl.BlockSpec(memory_space=pltpu.HBM)] * 3,
            out_specs=pl.BlockSpec(memory_space=pltpu.VMEM),
            scratch_shapes=[
                pltpu.VMEM(q.shape, q.dtype),
                pltpu.VMEM((SLOTS, tokens, heads, head), k.dtype),
                pltpu.VMEM((SLOTS, tokens, heads, head), v.dtype),
                pltpu.VMEM((heads, tokens * heads), jnp.float32),
                pltpu.VMEM((BEHIND, heads, tokens * heads), jnp.bfloat16),
                pltpu.VMEM((2, 2, heads, head), jnp.float32),
                pltpu.VMEM((2, heads, head), jnp.float32),
                pltpu.VMEM((n, heads, head), jnp.bfloat16),
                pltpu.VMEM((n, heads, 2 * LANES), jnp.float32),
                pltpu.VMEM((2, n, heads, head), jnp.bfloat16),
                pltpu.VMEM((2, n, heads, 2 * LANES), jnp.float32),
                pltpu.VMEM((2, heads, head), jnp.float32),
                pltpu.VMEM((2, heads, 2 * LANES), jnp.float32),
                pltpu.SemaphoreType.DMA,
                pltpu.SemaphoreType.DMA((SLOTS,)),
                pltpu.SemaphoreType.DMA((SLOTS,)),
                pltpu.SemaphoreType.DMA((2,)),
                pltpu.SemaphoreType.DMA((2, 2, 2)),
                pltpu.SemaphoreType.DMA((2,)),
            ],
            compiler_params=pltpu.CompilerParams(collective_id=0, has_side_effects=True, vmem_limit_bytes=67043328 - 192 * 1024),
        )(q, k, v)

    return jax.shard_map(
        step,
        mesh=mesh,
        in_specs=(P("dp", None, None), P("dp", "sp", None, None), P("dp", "sp", None, None)),
        out_specs=P("dp", None, None),
        check_vma=False,
    )
```
